32 devices in a mesh: row: 4 (over y, x), col: 8 (over z, core).
Axes of the slice: x: 2, y: 2, z: 4, core: 2. Of those that a mesh axis runs over, the one named last changes fastest.
Arguments:
- start_vector: bfloat16 [4, 2048, 2048], P(None, 'row', 'col'), may hold values from -150 to 150
- left_env: bfloat16 [5, 2048, 2048], P(None, 'row', 'col'), may hold values from -5 to 6
- right_env: bfloat16 [5, 2048, 2048], P(None, 'col', 'row'), may hold values from -5 to 6
- left_tensor: float32 [5, 5, 2, 2], replicated, may hold values from -1.5 to 2.5
- right_tensor: float32 [5, 5, 2, 2], replicated, may hold values from -1.5 to 2.5
Outputs:
- next_vector: bfloat16 [4, 2048, 2048], P(None, 'row', 'col')
- coefficients: float32 [2], replicated
The draws below stay inside these ranges and needn't reach their ends.
All inputs are finite; a program needn't handle non-finite values.
Results may differ from the reference program's by a relative error of at most 0.023.
Values may be sent and summed in bfloat16 or wider, within the bound.
A program may use at most 64 MiB of HBM per device.

```python
import jax
import jax.numpy as jnp
from jax import lax

D = 2048
CHANNELS = 5
STATES = 4
N_COL = 8


def environment(key, rising):
    random_part = jax.random.truncated_normal(key, -4.0, 4.0, (CHANNELS, D, D), jnp.float32)
    symmetric = (random_part + jnp.swapaxes(random_part, 1, 2)) * 0.5 ** 0.5 * D ** (-0.5)
    first_channel = (jnp.arange(CHANNELS) == 0).astype(jnp.float32)
    positions = jnp.arange(D, dtype=jnp.float32) / D
    diagonal_values = rising * (0.5 + 2.5 * positions) + (1.0 - rising) * jnp.ones((D,), jnp.float32)
    identity = jnp.eye(D, dtype=jnp.float32) * diagonal_values[:, None]
    return (symmetric + first_channel[:, None, None] * identity[None, :, :]).astype(jnp.bfloat16)


def site_tensor(key):
    raw_values = jax.random.truncated_normal(key, -4.0, 4.0, (CHANNELS, CHANNELS, 2, 2), jnp.float32)
    symmetric = (raw_values + jnp.swapaxes(raw_values, 2, 3)) * 0.5 * 0.3
    indices = jnp.arange(CHANNELS)
    corner = (indices == 0) | (indices == CHANNELS - 1)
    marks = ((indices[:, None] == indices[None, :]) & corner[:, None]).astype(jnp.float32)
    return symmetric + marks[:, :, None, None] * jnp.eye(2, dtype=jnp.float32)[None, None, :, :]


def draw_start_vector(key, part):
    positions = jnp.arange(D, dtype=jnp.float32) / D
    row_scale = jnp.exp(jax.random.uniform(jax.random.fold_in(key, 11), (D,), jnp.float32, -0.7, 0.7))
    col_scale = jnp.exp(jax.random.uniform(jax.random.fold_in(key, 12), (D,), jnp.float32, -0.7, 0.7))
    base_values = jax.random.truncated_normal(jax.random.fold_in(key, 13), -4.0, 4.0, (STATES, D, D), jnp.float32)
    row_scale = row_scale * (1.0 + 2.0 * positions)
    col_scale = col_scale * (1.0 + 2.0 * positions)
    return (base_values * row_scale[None, :, None] * col_scale[None, None, :]).astype(jnp.bfloat16)


def draw_left_env(key, part):
    return environment(jax.random.fold_in(key, 1), 1.0)


def draw_right_env(key, part):
    return environment(jax.random.fold_in(key, 2), 0.0)


def draw_left_tensor(key, part):
    return site_tensor(jax.random.fold_in(key, 3))


def draw_right_tensor(key, part):
    return site_tensor(jax.random.fold_in(key, 4))


def setup_inputs(seed: int = 0) -> dict:
    key_list = jax.random.split(jax.random.key(seed), 6)
    start_vector = draw_start_vector(jax.random.fold_in(key_list[5], 71), 0)
    left_env = draw_left_env(jax.random.fold_in(key_list[5], 71), 0)
    right_env = draw_right_env(jax.random.fold_in(key_list[5], 71), 0)
    left_tensor = draw_left_tensor(jax.random.fold_in(key_list[5], 71), 0)
    right_tensor = draw_right_tensor(jax.random.fold_in(key_list[5], 71), 0)
    return dict(start_vector=start_vector, left_env=left_env, right_env=right_env, left_tensor=left_tensor, right_tensor=right_tensor)


def coupling(left_tensor, right_tensor):
    channels = left_tensor.shape[0]
    joined = jnp.einsum('wuac,uvbd->vabwcd', left_tensor.astype(jnp.float32), right_tensor.astype(jnp.float32), precision=lax.Precision.HIGHEST)
    return joined.reshape(channels, 4, channels, 4)

def apply_hamiltonian(vector, coupling_table, left_env, right_env):
    cross = jnp.einsum('wax,txb->wtab', left_env.astype(jnp.float32), vector.astype(jnp.float32), precision=lax.Precision.HIGHEST)
    mixed_bond = jnp.einsum('vswt,wtab->vsab', coupling_table, cross, precision=lax.Precision.HIGHEST).astype(jnp.bfloat16)
    block_width = D // N_COL

    def accumulate(running, block_index):
        offset = block_index * block_width
        mixed_part = lax.dynamic_slice_in_dim(mixed_bond, offset, block_width, 3)
        right_part = lax.dynamic_slice_in_dim(right_env, offset, block_width, 1)
        partial_value = jnp.einsum('vsab,vbc->sac', mixed_part.astype(jnp.float32), right_part.astype(jnp.float32), precision=lax.Precision.HIGHEST)
        partial_value = lax.optimization_barrier(partial_value.astype(jnp.bfloat16)).astype(jnp.float32)
        return (running + partial_value, None)
    initial = jnp.zeros((vector.shape[0], D, D), jnp.float32)
    result, unused = lax.scan(accumulate, initial, jnp.arange(N_COL, dtype=jnp.int32))
    return result

def reference(start_vector, left_env, right_env, left_tensor, right_tensor):
    epsilon = 1e-06
    coupling_table = coupling(left_tensor, right_tensor)
    base_vector = start_vector.astype(jnp.float32)
    image = apply_hamiltonian(start_vector, coupling_table, left_env, right_env)
    base_square = jnp.mean(base_vector * base_vector)
    alpha = jnp.mean(base_vector * image) / (base_square + epsilon)
    residual = image - alpha * base_vector
    rho = jnp.sqrt(jnp.mean(residual * residual) + epsilon)
    next_vector = (residual / rho).astype(jnp.bfloat16)
    coefficients = jnp.stack([alpha, rho]).astype(jnp.float32)
    return (next_vector, coefficients)
```

```python
import functools

import jax
import jax.numpy as jnp
from jax import lax
from jax.experimental import pallas as pl
from jax.experimental.pallas import tpu as pltpu
from jax.sharding import PartitionSpec as P

epsilon = 1e-06
PIECES = 4
LAG = 2
MESH = pl.DeviceIdType.MESH


def coupling(left_tensor, right_tensor):
    channels = left_tensor.shape[0]
    joined = jnp.einsum(
        "wuac,uvbd->vabwcd", left_tensor, right_tensor, precision=lax.Precision.HIGHEST
    )
    return joined.reshape(channels, 4, channels, 4)


def contract_left(portion, columns):
    return jnp.einsum("wax,txb->wtba", portion, columns, preferred_element_type=jnp.float32)


def mix_channels(coupling_table, cross):
    mixed_bond = jnp.einsum(
        "vswt,wtba->vsba", coupling_table, cross, precision=lax.Precision.HIGHEST
    )
    return mixed_bond.astype(jnp.bfloat16)


def contract_right(mixed_bond, portion):
    return jnp.einsum("vsba,vbc->sac", mixed_bond, portion, preferred_element_type=jnp.float32)


def plain_image(start_vector, left_env, right_env, coupling_table):
    left_panel = lax.all_gather(left_env, "col", axis=2, tiled=True)
    right_panel = lax.all_gather(right_env, "row", axis=2, tiled=True)
    columns = lax.all_gather(start_vector, "row", axis=1, tiled=True)
    cross = contract_left(left_panel, columns)
    mixed_bond = mix_channels(coupling_table, cross)
    partials = contract_right(mixed_bond, right_panel)
    return lax.psum_scatter(
        partials.astype(jnp.bfloat16), "col", scatter_dimension=2, tiled=True
    ).astype(jnp.float32)


def image_kernel(
    layers, entries, table_ref, x_ref, l_ref, r_ref, next_ref, coef_ref,
    xg, lg, rg, cross, mixed, pair_out, pair_in, chain_out, chain_in, total, image, stat_out, stat_in,
    local_sem, l_send, l_recv, lp_send, lp_recv,
    g_send, g_recv, d_send, d_recv, p_send, p_recv, c_send, c_recv, s_send, s_recv,
):
    states, rows, width = x_ref.shape
    channels = l_ref.shape[0]
    piece = rows // PIECES
    row = lax.axis_index("row")
    col = lax.axis_index("col")
    layer = col // 2
    core = col % 2
    partner = (row, layer * 2 + (1 - core))
    above = (row, (layer + 1) * 2 + core)
    below = (row, (layer - 1) * 2 + core)
    ways = (above, below)
    sides = ((row // 2 * 2 + (1 - row % 2), col), (((row // 2) + 1) % 2 * 2 + row % 2, col))
    side_rows = (sides[0][0], sides[1][0])
    corner = ((row // 2) + 1) % 2 * 2 + (1 - row % 2)
    has = (layer < layers - 1, layer > 0)
    crossed = (row, ((layer + layers // 2) % layers) * 2 + core)
    beside = (row, (layer // 2 * 2 + (1 - layer % 2)) * 2 + core)
    rounds = (partner, beside, crossed) + sides

    def remote(src, dst, send, recv, device):
        return pltpu.make_async_remote_copy(
            src_ref=src, dst_ref=dst, send_sem=send, recv_sem=recv,
            device_id=device, device_id_type=MESH,
        )

    barrier = pltpu.get_barrier_semaphore()
    for device in (partner, crossed) + sides:
        pl.semaphore_signal(barrier, inc=1, device_id=device, device_id_type=MESH)
    for w in range(2):
        @pl.when(has[w])
        def _():
            pl.semaphore_signal(barrier, inc=1, device_id=ways[w], device_id_type=MESH)
    pl.semaphore_wait(barrier, 4 + jnp.minimum(layer, 1) + jnp.minimum(layers - 1 - layer, 1))

    def column(index, size):
        return pl.ds(pl.multiple_of(index * size, size), size)

    half = states // 2

    def own_part(which, part):
        if which == 0:
            return x_ref.at[pl.ds(part * half, half)]
        return r_ref.at[:, pl.ds(part * (width // 2), width // 2), :]

    def held_part(which, source, part):
        if which == 0:
            return xg.at[pl.ds(part * half, half), column(source, rows), :]
        return rg.at[source, :, pl.ds(part * (width // 2), width // 2), :]

    def side_copy(which, side, part):
        return remote(
            own_part(which, part), held_part(which, row, part),
            g_send.at[which, side, part], g_recv.at[which, side, part], sides[side],
        )

    def side_arrival(which, side, part):
        return remote(
            own_part(which, part), held_part(which, side_rows[side], part),
            g_send.at[which, side, part], g_recv.at[which, side, part], sides[side],
        )

    def relay_copy(which, side):
        part = held_part(which, side_rows[1 - side], side)
        return remote(part, part, d_send.at[which, side], d_recv.at[which, side], sides[side])

    def relay_arrival(which, side):
        part = held_part(which, corner, side)
        return remote(part, part, d_send.at[which, side], d_recv.at[which, side], sides[side])

    def start_sides(which):
        for side in range(2):
            side_copy(which, side, 1 - side).start()
        for side in range(2):
            side_copy(which, side, side).start()

    def start_relays(which):
        for side in range(2):
            side_arrival(which, 1 - side, side).wait_recv()
            relay_copy(which, side).start()

    def finish_sides(which):
        for side in range(2):
            side_arrival(which, side, side).wait_recv()

    def finish_corner(which):
        for side in range(2):
            relay_arrival(which, side).wait_recv()

    def own_left(k):
        return l_ref.at[:, column(k, piece), :]

    def held_left(k, owner):
        return lg.at[k, :, :, column(owner, width)]

    def left_copy(w, k, distance):
        owner = (layer - distance if w == 0 else layer + distance) * 2 + core
        source = own_left(k) if distance == 0 else held_left(k, owner)
        return remote(
            source, held_left(k, owner),
            l_send.at[w, distance, k], l_recv.at[w, distance, k], ways[w],
        )

    def left_arrival(w, k, distance):
        owner = (layer - distance if w == 0 else layer + distance) * 2 + core
        part = held_left(k, owner)
        return remote(
            part, part, l_send.at[w, distance - 1, k], l_recv.at[w, distance - 1, k], ways[w]
        )

    def pair_left(k, owner_layer, own):
        owner = owner_layer * 2 + core
        source = own_left(k) if own else held_left(k, owner)
        return remote(
            source, held_left(k, owner),
            lp_send.at[owner_layer, k], lp_recv.at[owner_layer, k], partner,
        )

    def pair_arrival(k, owner_layer):
        part = held_left(k, owner_layer * 2 + (1 - core))
        return remote(part, part, lp_send.at[owner_layer, k], lp_recv.at[owner_layer, k], partner)

    def start_left(k):
        for w in range(2):
            @pl.when(has[w])
            def _():
                left_copy(w, k, 0).start()
        pair_left(k, layer, True).start()

    def reach(w, distance):
        return layer >= distance if w == 0 else layer + distance < layers

    def relay_left(k):
        for distance in range(1, layers):
            for w in range(2):
                @pl.when(reach(w, distance))
                def _():
                    left_arrival(w, k, distance).wait_recv()
                    if distance < layers - 1:
                        @pl.when(has[w])
                        def _():
                            left_copy(w, k, distance).start()
                    pair_left(k, layer - distance if w == 0 else layer + distance, False).start()

    def own_copies():
        return (
            pltpu.make_async_copy(x_ref, xg.at[:, column(row, rows), :], local_sem.at[0]),
            pltpu.make_async_copy(r_ref, rg.at[row], local_sem.at[1]),
        )

    def own_left_copy(k):
        return pltpu.make_async_copy(own_left(k), held_left(k, col), local_sem.at[2 + k])

    def multiply_left(k):
        own_left_copy(k).wait()
        for owner_layer in range(layers):
            pair_arrival(k, owner_layer).wait_recv()

        def state_step(t, carry):
            left = lg[k].reshape(channels * piece, lg.shape[3])
            product = jnp.dot(left, xg[t], preferred_element_type=jnp.float32)
            cross[t] = product.reshape(channels, piece, width)
            return carry

        lax.fori_loop(0, states, state_step, 0)
        lanes = width // 128

        def mix_step(index, carry):
            at = pl.ds(pl.multiple_of(index // lanes * 16, 16), 16)
            lane = index % lanes * 128
            taken = [
                cross[t, w, at, pl.ds(pl.multiple_of(lane, 128), 128)]
                for w in range(channels) for t in range(states)
            ]
            for v in range(channels):
                for s in range(states):
                    base = (v * states + s) * channels * states
                    value = table_ref[base] * taken[0]
                    for n in range(1, channels * states):
                        value = value + table_ref[base + n] * taken[n]
                    spot = pl.ds(pl.multiple_of(v * width + lane, 128), 128)
                    mixed[k, s, at, spot] = value.astype(jnp.bfloat16)
            return carry

        lax.fori_loop(0, piece // 16 * lanes, mix_step, 0)

    def pair_term(unit):
        return remote(
            pair_out.at[unit], pair_in.at[unit], p_send.at[unit], p_recv.at[unit], partner
        )

    def chain_term(w, unit):
        return remote(
            chain_out.at[unit], chain_in.at[w, unit], c_send.at[unit], c_recv.at[w, unit], ways[w]
        )

    def product_right(k, target, side):
        left = mixed[k].reshape(states * piece, channels * width)
        right = rg[target, :, :, column(side, width)].reshape(channels * width, width)
        return jnp.dot(left, right, preferred_element_type=jnp.float32).reshape(
            states, piece, width
        )

    def target_of(unit):
        order = unit // PIECES
        return (row // 2 + order // 2) % 2 * 2 + (row + order) % 2

    slots = total.shape[0]

    def send_on(unit, target):
        for w in range(2):
            @pl.when(layer < target if w == 0 else layer > target)
            def _():
                chain_out[unit] = total[unit % slots].astype(jnp.bfloat16)
                chain_term(w, unit).start()

    def make_unit(unit):
        k = unit % PIECES
        target = target_of(unit)
        pair_out[unit] = product_right(k, target, 1 - core).astype(jnp.bfloat16)
        pair_term(unit).start()
        total[unit % slots] = product_right(k, target, core)
        pair_term(unit).wait_recv()
        total[unit % slots] += pair_in[unit].astype(jnp.float32)

    def join_unit(unit):
        k = unit % PIECES
        target = target_of(unit)
        slot = unit % slots
        for w in range(2):
            ahead = layer <= target if w == 0 else layer >= target

            @pl.when(has[1 - w] & ahead)
            def _():
                chain_term(w, unit).wait_recv()
                total[slot] += chain_in[w, unit].astype(jnp.float32)
        send_on(unit, target)

        @pl.when(layer == target)
        def _():
            image[:, column(k, piece), :] = total[slot]

    def join_step(step):
        for hops in range(layers - 1, -1, -1):
            unit = step - hops * LAG

            @pl.when((unit >= 0) & (unit < layers * PIECES))
            def _():
                target = target_of(unit)
                low = jnp.minimum(layer, layers - 1 - layer)
                high = layers - 1 - low
                up, down = layer, layers - 1 - layer
                fits = (
                    ((layer < target) & (up == hops))
                    | ((layer > target) & (down == hops))
                    | ((layer == target) & (high == hops))
                )

                @pl.when(fits)
                def _():
                    join_unit(unit)

    for copy in own_copies():
        copy.start()
    for k in range(PIECES):
        own_left_copy(k).start()
    start_left(0)
    start_sides(0)
    start_left(1)
    start_relays(0)
    start_sides(1)
    relay_left(0)
    start_left(2)
    finish_sides(0)
    finish_corner(0)
    for copy in own_copies():
        copy.wait()

    def piece_step(k, carry):
        @pl.when(k < PIECES - 1)
        def _():
            relay_left(k + 1)

        @pl.when(k < PIECES - 3)
        def _():
            start_left(k + 3)

        multiply_left(k)
        make_unit(k)
        join_step(k)

        @pl.when(k == 1)
        def _():
            start_relays(1)

        return carry

    lax.fori_loop(0, PIECES, piece_step, 0)
    finish_sides(1)

    def unit_step(unit, carry):
        @pl.when(unit == 3 * PIECES)
        def _():
            finish_corner(1)

        @pl.when(unit < layers * PIECES)
        def _():
            make_unit(unit)

        join_step(unit)
        return carry

    lax.fori_loop(PIECES, layers * PIECES + (layers - 1) * LAG, unit_step, 0)

    def sum_step(index, sums):
        at = pl.ds(pl.multiple_of(index * 8, 8), 8)
        base_square, correlation, image_square = sums
        for t in range(states):
            former = x_ref[t, at, :].astype(jnp.float32)
            latter = image[t, at, :]
            base_square = base_square + former * former
            correlation = correlation + former * latter
            image_square = image_square + latter * latter
        return base_square, correlation, image_square

    nothing = jnp.zeros((8, width), jnp.float32)
    sums = lax.fori_loop(0, rows // 8, sum_step, (nothing, nothing, nothing))
    for n in range(3):
        stat_out[0, n] = jnp.sum(sums[n].reshape(8, width // 128, 128), axis=1) / entries
    for number, device in enumerate(rounds):
        swap = remote(
            stat_out.at[number], stat_in.at[number], s_send.at[number], s_recv.at[number], device
        )
        swap.start()
        swap.wait_recv()
        stat_out[number + 1] = stat_out[number] + stat_in[number]
    base_square, correlation, image_square = (
        jnp.sum(stat_out[len(rounds), n], axis=(0, 1), keepdims=True) for n in range(3)
    )
    alpha = correlation / (base_square + epsilon)
    square = image_square - 2.0 * alpha * correlation + alpha * alpha * base_square
    rho = jnp.sqrt(square + epsilon)
    coef_ref[0] = jnp.broadcast_to(alpha, (8, 128))
    coef_ref[1] = jnp.broadcast_to(rho, (8, 128))

    def scale_step(index, carry):
        at = pl.ds(pl.multiple_of(index * 16, 16), 16)
        for t in range(states):
            residual = image[t, at, :] - alpha * x_ref[t, at, :].astype(jnp.float32)
            next_ref[t, at, :] = (residual / rho).astype(jnp.bfloat16)
        return carry

    lax.fori_loop(0, rows // 16, scale_step, 0)
    for number, device in enumerate(rounds):
        remote(
            stat_out.at[number], stat_in.at[number], s_send.at[number], s_recv.at[number], device
        ).wait_send()

    for which in range(2):
        for side in range(2):
            side_copy(which, side, 0).wait_send()
            side_copy(which, side, 1).wait_send()
            relay_copy(which, side).wait_send()

    def left_end(k, carry):
        pair_left(k, layer, True).wait_send()
        for w in range(2):
            @pl.when(has[w])
            def _():
                left_copy(w, k, 0).wait_send()
        for distance in range(1, layers):
            for w in range(2):
                @pl.when(reach(w, distance))
                def _():
                    if distance < layers - 1:
                        @pl.when(has[w])
                        def _():
                            left_copy(w, k, distance).wait_send()
                    pair_left(k, layer - distance if w == 0 else layer + distance, False).wait_send()
        return carry

    lax.fori_loop(0, PIECES, left_end, 0)

    def unit_end(unit, carry):
        target = target_of(unit)
        pair_term(unit).wait_send()
        for w in range(2):
            @pl.when(layer < target if w == 0 else layer > target)
            def _():
                chain_term(w, unit).wait_send()
        return carry

    lax.fori_loop(0, 4 * PIECES, unit_end, 0)


def linked_step(start_vector, left_env, right_env, coupling_table, entries):
    states, rows, width = start_vector.shape
    channels = left_env.shape[0]
    sources = lax.axis_size("row")
    owners = lax.axis_size("col")
    layers = owners // 2
    piece = rows // PIECES
    units = layers * PIECES
    narrow = jnp.bfloat16
    dma = pltpu.SemaphoreType.DMA
    return pl.pallas_call(
        functools.partial(image_kernel, layers, entries),
        out_shape=(
            jax.ShapeDtypeStruct((states, rows, width), narrow),
            jax.ShapeDtypeStruct((2, 8, 128), jnp.float32),
        ),
        in_specs=[pl.BlockSpec(memory_space=pltpu.SMEM)]
        + [pl.BlockSpec(memory_space=pltpu.VMEM)] * 3,
        out_specs=(pl.BlockSpec(memory_space=pltpu.VMEM),) * 2,
        scratch_shapes=[
            pltpu.VMEM((states, sources * rows, width), narrow),
            pltpu.VMEM((PIECES, channels, piece, owners * width), narrow),
            pltpu.VMEM((sources, channels, width, right_env.shape[2]), narrow),
            pltpu.VMEM((states, channels, piece, width), jnp.float32),
            pltpu.VMEM((PIECES, states, piece, channels * width), narrow),
            pltpu.VMEM((units, states, piece, width), narrow),
            pltpu.VMEM((units, states, piece, width), narrow),
            pltpu.VMEM((units, states, piece, width), narrow),
            pltpu.VMEM((2, units, states, piece, width), narrow),
            pltpu.VMEM((8, states, piece, width), jnp.float32),
            pltpu.VMEM((states, rows, width), jnp.float32),
            pltpu.VMEM((6, 3, 8, 128), jnp.float32),
            pltpu.VMEM((5, 3, 8, 128), jnp.float32),
            dma((2 + PIECES,)),
            dma((2, layers, PIECES)),
            dma((2, layers, PIECES)),
            dma((layers, PIECES)),
            dma((layers, PIECES)),
            dma((2, 2, 2)),
            dma((2, 2, 2)),
            dma((2, 2)),
            dma((2, 2)),
            dma((units,)),
            dma((units,)),
            dma((units,)),
            dma((2, units)),
            dma((5,)),
            dma((5,)),
        ],
        compiler_params=pltpu.CompilerParams(
            collective_id=0, has_side_effects=True, vmem_limit_bytes=65000 * 1024
        ),
    )(coupling_table.reshape(-1), start_vector, left_env, right_env)


def local_mean(former, latter, entries):
    return jnp.sum(former * latter) / entries


def body(start_vector, left_env, right_env, left_tensor, right_tensor):
    coupling_table = coupling(left_tensor, right_tensor)
    states, rows, width = start_vector.shape
    sources = lax.axis_size("row")
    owners = lax.axis_size("col")
    entries = float(states * rows * width * sources * owners)
    planned = (
        sources == 4 and owners == 2 * sources and width % 128 == 0
        and rows % (PIECES * 16) == 0 and states % 2 == 0
    )
    if planned:
        next_vector, numbers = linked_step(
            start_vector, left_env, right_env, coupling_table, entries
        )
        return (next_vector, numbers[:, 0, 0])
    base_vector = start_vector.astype(jnp.float32)
    image = plain_image(start_vector, left_env, right_env, coupling_table)
    base_square, correlation, image_square = lax.psum(
        (
            local_mean(base_vector, base_vector, entries),
            local_mean(base_vector, image, entries),
            local_mean(image, image, entries),
        ),
        ("row", "col"),
    )
    alpha = correlation / (base_square + epsilon)
    residual = image - alpha * base_vector
    rho = jnp.sqrt(image_square - 2.0 * alpha * correlation + alpha * alpha * base_square + epsilon)
    next_vector = (residual / rho).astype(jnp.bfloat16)
    coefficients = jnp.stack([alpha, rho])
    return (next_vector, coefficients)


def solution(mesh):
    return jax.shard_map(
        body,
        mesh=mesh,
        in_specs=(P(None, "row", "col"), P(None, "row", "col"), P(None, "col", "row"), P(), P()),
        out_specs=(P(None, "row", "col"), P()),
        check_vma=False,
    )
```

```python
import functools

import jax
import jax.numpy as jnp
from jax import lax
from jax.experimental import pallas as pl
from jax.experimental.pallas import tpu as pltpu
from jax.sharding import PartitionSpec as P

epsilon = 1e-06
PIECES = 4
LAG = 2
MESH = pl.DeviceIdType.MESH


def coupling(left_tensor, right_tensor):
    channels = left_tensor.shape[0]
    joined = jnp.einsum(
        "wuac,uvbd->vabwcd", left_tensor, right_tensor, precision=lax.Precision.HIGHEST
    )
    return joined.reshape(channels, 4, channels, 4)


def contract_left(portion, columns):
    return jnp.einsum("wax,txb->wtba", portion, columns, preferred_element_type=jnp.float32)


def mix_channels(coupling_table, cross):
    mixed_bond = jnp.einsum(
        "vswt,wtba->vsba", coupling_table, cross, precision=lax.Precision.HIGHEST
    )
    return mixed_bond.astype(jnp.bfloat16)


def contract_right(mixed_bond, portion):
    return jnp.einsum("vsba,vbc->sac", mixed_bond, portion, preferred_element_type=jnp.float32)


def plain_image(start_vector, left_env, right_env, coupling_table):
    left_panel = lax.all_gather(left_env, "col", axis=2, tiled=True)
    right_panel = lax.all_gather(right_env, "row", axis=2, tiled=True)
    columns = lax.all_gather(start_vector, "row", axis=1, tiled=True)
    cross = contract_left(left_panel, columns)
    mixed_bond = mix_channels(coupling_table, cross)
    partials = contract_right(mixed_bond, right_panel)
    return lax.psum_scatter(
        partials.astype(jnp.bfloat16), "col", scatter_dimension=2, tiled=True
    ).astype(jnp.float32)


def image_kernel(
    layers, entries, table_ref, x_ref, l_ref, r_ref, next_ref, coef_ref,
    xg, lg, rg, cross, mixed, pair_out, pair_in, chain_out, chain_in, total, image, stat_out, stat_in,
    local_sem, l_send, l_recv, lp_send, lp_recv,
    g_send, g_recv, d_send, d_recv, p_send, p_recv, c_send, c_recv, s_send, s_recv,
):
    states, rows, width = x_ref.shape
    channels = l_ref.shape[0]
    piece = rows // PIECES
    row = lax.axis_index("row")
    col = lax.axis_index("col")
    layer = col // 2
    core = col % 2
    partner = (row, layer * 2 + (1 - core))
    above = (row, (layer + 1) * 2 + core)
    below = (row, (layer - 1) * 2 + core)
    ways = (above, below)
    sides = ((row // 2 * 2 + (1 - row % 2), col), (((row // 2) + 1) % 2 * 2 + row % 2, col))
    side_rows = (sides[0][0], sides[1][0])
    corner = ((row // 2) + 1) % 2 * 2 + (1 - row % 2)
    has = (layer < layers - 1, layer > 0)
    crossed = (row, ((layer + layers // 2) % layers) * 2 + core)
    beside = (row, (layer // 2 * 2 + (1 - layer % 2)) * 2 + core)
    rounds = (partner, beside, crossed) + sides

    def remote(src, dst, send, recv, device):
        return pltpu.make_async_remote_copy(
            src_ref=src, dst_ref=dst, send_sem=send, recv_sem=recv,
            device_id=device, device_id_type=MESH,
        )

    barrier = pltpu.get_barrier_semaphore()
    for device in (partner, crossed) + sides:
        pl.semaphore_signal(barrier, inc=1, device_id=device, device_id_type=MESH)
    for w in range(2):
        @pl.when(has[w])
        def _():
            pl.semaphore_signal(barrier, inc=1, device_id=ways[w], device_id_type=MESH)
    pl.semaphore_wait(barrier, 4 + jnp.minimum(layer, 1) + jnp.minimum(layers - 1 - layer, 1))

    def column(index, size):
        return pl.ds(pl.multiple_of(index * size, size), size)

    half = states // 2

    def own_part(which, part):
        if which == 0:
            return x_ref.at[pl.ds(part * half, half)]
        return r_ref.at[:, pl.ds(part * (width // 2), width // 2), :]

    def held_part(which, source, part):
        if which == 0:
            return xg.at[pl.ds(part * half, half), column(source, rows), :]
        return rg.at[source, :, pl.ds(part * (width // 2), width // 2), :]

    def side_copy(which, side, part):
        return remote(
            own_part(which, part), held_part(which, row, part),
            g_send.at[which, side, part], g_recv.at[which, side, part], sides[side],
        )

    def side_arrival(which, side, part):
        return remote(
            own_part(which, part), held_part(which, side_rows[side], part),
            g_send.at[which, side, part], g_recv.at[which, side, part], sides[side],
        )

    def relay_copy(which, side):
        part = held_part(which, side_rows[1 - side], side)
        return remote(part, part, d_send.at[which, side], d_recv.at[which, side], sides[side])

    def relay_arrival(which, side):
        part = held_part(which, corner, side)
        return remote(part, part, d_send.at[which, side], d_recv.at[which, side], sides[side])

    def start_sides(which):
        for side in range(2):
            side_copy(which, side, 1 - side).start()
        for side in range(2):
            side_copy(which, side, side).start()

    def start_relays(which):
        for side in range(2):
            side_arrival(which, 1 - side, side).wait_recv()
            relay_copy(which, side).start()

    def finish_sides(which):
        for side in range(2):
            side_arrival(which, side, side).wait_recv()

    def finish_corner(which):
        for side in range(2):
            relay_arrival(which, side).wait_recv()

    def own_left(k):
        return l_ref.at[:, column(k, piece), :]

    def held_left(k, owner):
        return lg.at[k, :, :, column(owner, width)]

    def left_copy(w, k, distance):
        owner = (layer - distance if w == 0 else layer + distance) * 2 + core
        source = own_left(k) if distance == 0 else held_left(k, owner)
        return remote(
            source, held_left(k, owner),
            l_send.at[w, distance, k], l_recv.at[w, distance, k], ways[w],
        )

    def left_arrival(w, k, distance):
        owner = (layer - distance if w == 0 else layer + distance) * 2 + core
        part = held_left(k, owner)
        return remote(
            part, part, l_send.at[w, distance - 1, k], l_recv.at[w, distance - 1, k], ways[w]
        )

    def pair_left(k, owner_layer, own):
        owner = owner_layer * 2 + core
        source = own_left(k) if own else held_left(k, owner)
        return remote(
            source, held_left(k, owner),
            lp_send.at[owner_layer, k], lp_recv.at[owner_layer, k], partner,
        )

    def pair_arrival(k, owner_layer):
        part = held_left(k, owner_layer * 2 + (1 - core))
        return remote(part, part, lp_send.at[owner_layer, k], lp_recv.at[owner_layer, k], partner)

    def start_left(k):
        for w in range(2):
            @pl.when(has[w])
            def _():
                left_copy(w, k, 0).start()
        pair_left(k, layer, True).start()

    def reach(w, distance):
        return layer >= distance if w == 0 else layer + distance < layers

    def relay_hop(k, distance):
        for w in range(2):
            @pl.when(reach(w, distance))
            def _():
                left_arrival(w, k, distance).wait_recv()
                if distance < layers - 1:
                    @pl.when(has[w])
                    def _():
                        left_copy(w, k, distance).start()
                pair_left(k, layer - distance if w == 0 else layer + distance, False).start()

    def relay_later(k, distance):
        @pl.when(k < PIECES)
        def _():
            relay_hop(k, distance)

    def own_copies():
        return (
            pltpu.make_async_copy(x_ref, xg.at[:, column(row, rows), :], local_sem.at[0]),
            pltpu.make_async_copy(r_ref, rg.at[row], local_sem.at[1]),
        )

    def own_left_copy(k):
        return pltpu.make_async_copy(own_left(k), held_left(k, col), local_sem.at[2 + k])

    def multiply_left(k):
        own_left_copy(k).wait()
        for owner_layer in range(layers):
            pair_arrival(k, owner_layer).wait_recv()

        def state_step(t, carry):
            left = lg[k].reshape(channels * piece, lg.shape[3])
            product = jnp.dot(left, xg[t], preferred_element_type=jnp.float32)
            cross[t] = product.reshape(channels, piece, width)
            return carry

        lax.fori_loop(0, states, state_step, 0)
        for distance in range(2, layers - 1):
            relay_later(k + 1, distance)
        lanes = width // 128

        def mix_step(index, carry):
            at = pl.ds(pl.multiple_of(index // lanes * 16, 16), 16)
            lane = index % lanes * 128
            taken = [
                cross[t, w, at, pl.ds(pl.multiple_of(lane, 128), 128)]
                for w in range(channels) for t in range(states)
            ]
            for v in range(channels):
                for s in range(states):
                    base = (v * states + s) * channels * states
                    value = table_ref[base] * taken[0]
                    for n in range(1, channels * states):
                        value = value + table_ref[base + n] * taken[n]
                    spot = pl.ds(pl.multiple_of(v * width + lane, 128), 128)
                    mixed[k, s, at, spot] = value.astype(jnp.bfloat16)
            return carry

        lax.fori_loop(0, piece // 16 * lanes, mix_step, 0)

    def pair_term(unit):
        return remote(
            pair_out.at[unit], pair_in.at[unit], p_send.at[unit], p_recv.at[unit], partner
        )

    def chain_term(w, unit):
        return remote(
            chain_out.at[unit], chain_in.at[w, unit], c_send.at[unit], c_recv.at[w, unit], ways[w]
        )

    def product_right(k, target, side):
        left = mixed[k].reshape(states * piece, channels * width)
        right = rg[target, :, :, column(side, width)].reshape(channels * width, width)
        return jnp.dot(left, right, preferred_element_type=jnp.float32).reshape(
            states, piece, width
        )

    def target_of(unit):
        order = unit // PIECES
        return (row // 2 + order // 2) % 2 * 2 + (row + order) % 2

    slots = total.shape[0]

    def send_on(unit, target):
        for w in range(2):
            @pl.when(layer < target if w == 0 else layer > target)
            def _():
                chain_out[unit] = total[unit % slots].astype(jnp.bfloat16)
                chain_term(w, unit).start()

    def make_unit(unit):
        k = unit % PIECES
        target = target_of(unit)
        pair_out[unit] = product_right(k, target, 1 - core).astype(jnp.bfloat16)
        pair_term(unit).start()
        total[unit % slots] = product_right(k, target, core)
        pair_term(unit).wait_recv()
        total[unit % slots] += pair_in[unit].astype(jnp.float32)

    def join_unit(unit):
        k = unit % PIECES
        target = target_of(unit)
        slot = unit % slots
        for w in range(2):
            ahead = layer <= target if w == 0 else layer >= target

            @pl.when(has[1 - w] & ahead)
            def _():
                chain_term(w, unit).wait_recv()
                total[slot] += chain_in[w, unit].astype(jnp.float32)
        send_on(unit, target)

        @pl.when(layer == target)
        def _():
            image[:, column(k, piece), :] = total[slot]

    def join_step(step):
        for hops in range(layers - 1, -1, -1):
            unit = step - hops * LAG

            @pl.when((unit >= 0) & (unit < layers * PIECES))
            def _():
                target = target_of(unit)
                low = jnp.minimum(layer, layers - 1 - layer)
                high = layers - 1 - low
                up, down = layer, layers - 1 - layer
                fits = (
                    ((layer < target) & (up == hops))
                    | ((layer > target) & (down == hops))
                    | ((layer == target) & (high == hops))
                )

                @pl.when(fits)
                def _():
                    join_unit(unit)

    for copy in own_copies():
        copy.start()
    for k in range(PIECES):
        own_left_copy(k).start()
    start_left(0)
    start_sides(0)
    start_left(1)
    start_relays(0)
    start_sides(1)
    for distance in range(1, layers):
        relay_hop(0, distance)
    start_left(2)
    finish_sides(0)
    finish_corner(0)
    for copy in own_copies():
        copy.wait()

    def piece_step(k, carry):
        relay_later(k + 1, 1)

        @pl.when(k < PIECES - 3)
        def _():
            start_left(k + 3)

        multiply_left(k)
        relay_later(k + 1, layers - 1)
        make_unit(k)
        join_step(k)

        @pl.when(k == 1)
        def _():
            start_relays(1)

        return carry

    lax.fori_loop(0, PIECES, piece_step, 0)
    finish_sides(1)

    def unit_step(unit, carry):
        @pl.when(unit == 3 * PIECES)
        def _():
            finish_corner(1)

        @pl.when(unit < layers * PIECES)
        def _():
            make_unit(unit)

        join_step(unit)
        return carry

    lax.fori_loop(PIECES, layers * PIECES + (layers - 1) * LAG, unit_step, 0)

    def sum_step(index, sums):
        at = pl.ds(pl.multiple_of(index * 8, 8), 8)
        base_square, correlation, image_square = sums
        for t in range(states):
            former = x_ref[t, at, :].astype(jnp.float32)
            latter = image[t, at, :]
            base_square = base_square + former * former
            correlation = correlation + former * latter
            image_square = image_square + latter * latter
        return base_square, correlation, image_square

    nothing = jnp.zeros((8, width), jnp.float32)
    sums = lax.fori_loop(0, rows // 8, sum_step, (nothing, nothing, nothing))
    for n in range(3):
        stat_out[0, n] = jnp.sum(sums[n].reshape(8, width // 128, 128), axis=1) / entries
    for number, device in enumerate(rounds):
        swap = remote(
            stat_out.at[number], stat_in.at[number], s_send.at[number], s_recv.at[number], device
        )
        swap.start()
        swap.wait_recv()
        stat_out[number + 1] = stat_out[number] + stat_in[number]
    base_square, correlation, image_square = (
        jnp.sum(stat_out[len(rounds), n], axis=(0, 1), keepdims=True) for n in range(3)
    )
    alpha = correlation / (base_square + epsilon)
    square = image_square - 2.0 * alpha * correlation + alpha * alpha * base_square
    rho = jnp.sqrt(square + epsilon)
    coef_ref[0] = jnp.broadcast_to(alpha, (8, 128))
    coef_ref[1] = jnp.broadcast_to(rho, (8, 128))

    def scale_step(index, carry):
        at = pl.ds(pl.multiple_of(index * 16, 16), 16)
        for t in range(states):
            residual = image[t, at, :] - alpha * x_ref[t, at, :].astype(jnp.float32)
            next_ref[t, at, :] = (residual / rho).astype(jnp.bfloat16)
        return carry

    lax.fori_loop(0, rows // 16, scale_step, 0)
    for number, device in enumerate(rounds):
        remote(
            stat_out.at[number], stat_in.at[number], s_send.at[number], s_recv.at[number], device
        ).wait_send()

    for which in range(2):
        for side in range(2):
            side_copy(which, side, 0).wait_send()
            side_copy(which, side, 1).wait_send()
            relay_copy(which, side).wait_send()

    def left_end(k, carry):
        pair_left(k, layer, True).wait_send()
        for w in range(2):
            @pl.when(has[w])
            def _():
                left_copy(w, k, 0).wait_send()
        for distance in range(1, layers):
            for w in range(2):
                @pl.when(reach(w, distance))
                def _():
                    if distance < layers - 1:
                        @pl.when(has[w])
                        def _():
                            left_copy(w, k, distance).wait_send()
                    pair_left(k, layer - distance if w == 0 else layer + distance, False).wait_send()
        return carry

    lax.fori_loop(0, PIECES, left_end, 0)

    def unit_end(unit, carry):
        target = target_of(unit)
        pair_term(unit).wait_send()
        for w in range(2):
            @pl.when(layer < target if w == 0 else layer > target)
            def _():
                chain_term(w, unit).wait_send()
        return carry

    lax.fori_loop(0, 4 * PIECES, unit_end, 0)


def linked_step(start_vector, left_env, right_env, coupling_table, entries):
    states, rows, width = start_vector.shape
    channels = left_env.shape[0]
    sources = lax.axis_size("row")
    owners = lax.axis_size("col")
    layers = owners // 2
    piece = rows // PIECES
    units = layers * PIECES
    narrow = jnp.bfloat16
    dma = pltpu.SemaphoreType.DMA
    return pl.pallas_call(
        functools.partial(image_kernel, layers, entries),
        out_shape=(
            jax.ShapeDtypeStruct((states, rows, width), narrow),
            jax.ShapeDtypeStruct((2, 8, 128), jnp.float32),
        ),
        in_specs=[pl.BlockSpec(memory_space=pltpu.SMEM)]
        + [pl.BlockSpec(memory_space=pltpu.VMEM)] * 3,
        out_specs=(pl.BlockSpec(memory_space=pltpu.VMEM),) * 2,
        scratch_shapes=[
            pltpu.VMEM((states, sources * rows, width), narrow),
            pltpu.VMEM((PIECES, channels, piece, owners * width), narrow),
            pltpu.VMEM((sources, channels, width, right_env.shape[2]), narrow),
            pltpu.VMEM((states, channels, piece, width), jnp.float32),
            pltpu.VMEM((PIECES, states, piece, channels * width), narrow),
            pltpu.VMEM((units, states, piece, width), narrow),
            pltpu.VMEM((units, states, piece, width), narrow),
            pltpu.VMEM((units, states, piece, width), narrow),
            pltpu.VMEM((2, units, states, piece, width), narrow),
            pltpu.VMEM((8, states, piece, width), jnp.float32),
            pltpu.VMEM((states, rows, width), jnp.float32),
            pltpu.VMEM((6, 3, 8, 128), jnp.float32),
            pltpu.VMEM((5, 3, 8, 128), jnp.float32),
            dma((2 + PIECES,)),
            dma((2, layers, PIECES)),
            dma((2, layers, PIECES)),
            dma((layers, PIECES)),
            dma((layers, PIECES)),
            dma((2, 2, 2)),
            dma((2, 2, 2)),
            dma((2, 2)),
            dma((2, 2)),
            dma((units,)),
            dma((units,)),
            dma((units,)),
            dma((2, units)),
            dma((5,)),
            dma((5,)),
        ],
        compiler_params=pltpu.CompilerParams(
            collective_id=0, has_side_effects=True, vmem_limit_bytes=65000 * 1024
        ),
    )(coupling_table.reshape(-1), start_vector, left_env, right_env)


def local_mean(former, latter, entries):
    return jnp.sum(former * latter) / entries


def body(start_vector, left_env, right_env, left_tensor, right_tensor):
    coupling_table = coupling(left_tensor, right_tensor)
    states, rows, width = start_vector.shape
    sources = lax.axis_size("row")
    owners = lax.axis_size("col")
    entries = float(states * rows * width * sources * owners)
    planned = (
        sources == 4 and owners == 2 * sources and width % 128 == 0
        and rows % (PIECES * 16) == 0 and states % 2 == 0
    )
    if planned:
        next_vector, numbers = linked_step(
            start_vector, left_env, right_env, coupling_table, entries
        )
        return (next_vector, numbers[:, 0, 0])
    base_vector = start_vector.astype(jnp.float32)
    image = plain_image(start_vector, left_env, right_env, coupling_table)
    base_square, correlation, image_square = lax.psum(
        (
            local_mean(base_vector, base_vector, entries),
            local_mean(base_vector, image, entries),
            local_mean(image, image, entries),
        ),
        ("row", "col"),
    )
    alpha = correlation / (base_square + epsilon)
    residual = image - alpha * base_vector
    rho = jnp.sqrt(image_square - 2.0 * alpha * correlation + alpha * alpha * base_square + epsilon)
    next_vector = (residual / rho).astype(jnp.bfloat16)
    coefficients = jnp.stack([alpha, rho])
    return (next_vector, coefficients)


def solution(mesh):
    return jax.shard_map(
        body,
        mesh=mesh,
        in_specs=(P(None, "row", "col"), P(None, "row", "col"), P(None, "col", "row"), P(), P()),
        out_specs=(P(None, "row", "col"), P()),
        check_vma=False,
    )
```
